32 devices in a mesh: dp: 4 (over x, y), tp: 8 (over z, core).
Axes of the slice: x: 2, y: 2, z: 4, core: 2. Of those that a mesh axis runs over, the one named last changes fastest.
Arguments:
- x: bfloat16 [16, 512, 5120], P('dp'), parts along dimension 0
- gain_a: bfloat16 [5120], replicated
- wq: bfloat16 [5120, 4096], P(None, 'tp')
- wk: bfloat16 [5120, 1024], P(None, 'tp')
- wv: bfloat16 [5120, 1024], P(None, 'tp')
- wo: bfloat16 [4096, 5120], P('tp')
- gain_m: bfloat16 [5120], replicated
- w_gate: bfloat16 [5120, 14336], P(None, 'tp')
- w_up: bfloat16 [5120, 14336], P(None, 'tp')
- w_down: bfloat16 [14336, 5120], P('tp')
Outputs:
- output: bfloat16 [16, 512, 5120], P('dp'), parts along dimension 0
There are 4 independent parts. The reference program is written for one: setup_inputs(seed, part) draws one part's arguments, and reference() takes and returns one part's arrays. A program takes and returns all parts, laid end to end along the dimension named above; an argument that names none is the same for every part.
All inputs are finite; a program needn't handle non-finite values.
Results may differ from the reference program's by a relative error of at most 0.017.
Values are sent between devices in bfloat16 or wider.
A program may use at most 2 GiB of HBM per device.

```python
import jax
import jax.numpy as jnp
from jax import lax

SEQUENCES = 4
TOKENS = 512
D = 5120
HEADS = 32
KV_HEADS = 8
HEAD = 128
FF = 14336
THETA = 10000


def setup_inputs(seed: int = 0, part: int = 0) -> dict:
    kx, ka, km, kq, kk, kv, ko, kg, ku, kd = jax.random.split(jax.random.key(seed), 10)

    def weights(key, rows, columns):
        return jax.random.normal(key, (rows, columns), jnp.float32) * rows**-0.5

    drawn = {
        "x": jax.random.normal(jax.random.fold_in(kx, part), (SEQUENCES, TOKENS, D), jnp.float32),
        "gain_a": 1 + 0.1 * jax.random.normal(ka, (D,), jnp.float32),
        "wq": 2 * weights(kq, D, HEADS * HEAD),
        "wk": 2 * weights(kk, D, KV_HEADS * HEAD),
        "wv": 4 * weights(kv, D, KV_HEADS * HEAD),
        "wo": weights(ko, HEADS * HEAD, D),
        "gain_m": 1 + 0.1 * jax.random.normal(km, (D,), jnp.float32),
        "w_gate": weights(kg, D, FF),
        "w_up": weights(ku, D, FF),
        "w_down": 3 * weights(kd, FF, D),
    }
    return {k: v.astype(jnp.bfloat16) for k, v in drawn.items()}


def normed(x, gain):
    wide = x.astype(jnp.float32)
    scale = lax.rsqrt(jnp.mean(wide * wide, -1, keepdims=True) + 1e-6)
    return (wide * scale * gain.astype(jnp.float32)).astype(jnp.bfloat16)


def turned(t, place, theta):
    half = t.shape[-1] // 2
    angle = place.astype(jnp.float32)[:, None] * theta ** (-jnp.arange(half, dtype=jnp.float32) / half)
    cos, sin = jnp.cos(angle)[:, None], jnp.sin(angle)[:, None]
    a, b = t[..., :half].astype(jnp.float32), t[..., half:].astype(jnp.float32)
    return jnp.concatenate([a * cos - b * sin, b * cos + a * sin], -1).astype(jnp.bfloat16)


def matmul(a, w):
    return jnp.dot(a, w, preferred_element_type=jnp.float32).astype(jnp.bfloat16)


def einsum(form, a, b):
    return jnp.einsum(form, a.astype(jnp.float32), b.astype(jnp.float32))


def attention(q, k, v):
    scores = einsum("tgsd,ugd->gstu", q, k) * q.shape[-1] ** -0.5
    token = jnp.arange(q.shape[0])
    scores = jnp.where(token[:, None] >= token, scores, -jnp.inf)
    weights = jax.nn.softmax(scores, -1).astype(jnp.bfloat16)
    return einsum("gstu,ugd->tgsd", weights, v).astype(jnp.bfloat16)


def one(x, gain_a, wq, wk, wv, wo, gain_m, w_gate, w_up, w_down):
    rows = x.shape[0]
    a, place = normed(x, gain_a), jnp.arange(rows)
    k = turned(matmul(a, wk).reshape(rows, -1, HEAD), place, THETA)
    q = turned(matmul(a, wq).reshape(rows, -1, HEAD), place, THETA).reshape(rows, k.shape[1], -1, HEAD)
    v = matmul(a, wv).reshape(rows, -1, HEAD)
    seen = attention(q, k, v).reshape(rows, -1)
    h = (x.astype(jnp.float32) + jnp.dot(seen, wo, preferred_element_type=jnp.float32)).astype(jnp.bfloat16)
    b = normed(h, gain_m)
    gate = jnp.dot(b, w_gate, preferred_element_type=jnp.float32)
    up = jnp.dot(b, w_up, preferred_element_type=jnp.float32)
    hidden = (jax.nn.silu(gate) * up).astype(jnp.bfloat16)
    return (h.astype(jnp.float32) + jnp.dot(hidden, w_down, preferred_element_type=jnp.float32)).astype(jnp.bfloat16)


def reference(x, gain_a, wq, wk, wv, wo, gain_m, w_gate, w_up, w_down):
    return lax.map(lambda sequence: one(sequence, gain_a, wq, wk, wv, wo, gain_m, w_gate, w_up, w_down), x)
```

```python
import functools

import jax
import jax.numpy as jnp
import numpy as np
from jax import lax
from jax.experimental import pallas as pl
from jax.experimental.pallas import tpu as pltpu
from jax.sharding import PartitionSpec as P

HEAD = 128
THETA = 10000
MESH = pl.DeviceIdType.MESH
CHIPS = 4
T = 256
HALF = T // 2
QUARTER = T // 4
PIECES = 4
ROWS = QUARTER // PIECES
HOP = 2
K = 8
LEAD = 4
R1, A1, R2, A2 = range(4)
JOBS = [(R1, 0), (R1, 1), (A1, 0), (R1, 2), (A1, 1), (R1, 3), (A1, 2), (R2, 0), (A1, 3), (R1, 4), (A2, 0), (R2, 1), (R1, 5), (A1, 4),
        (R2, 2), (A2, 1), (R1, 6), (A1, 5), (R2, 3), (R1, 7), (A1, 6), (R2, 4), (A1, 7), (R2, 5), (A2, 2), (R2, 6), (A2, 3), (R2, 7),
        (A2, 4), (A2, 5), (A2, 6), (A2, 7)]
NJ = len(JOBS) * PIECES
NS = NJ + HOP * (CHIPS - 1)
NB = 3
VMEM = 67_043_328


def pick(index, table):
    out = jnp.int32(0)
    for n, value in enumerate(table):
        if value:
            out += jnp.where(index == n, jnp.int32(value), jnp.int32(0))
    return out


def spread(total, count):
    return [total * (n + 1) // count - total * n // count for n in range(count)]


def kernel(x, wq, wk, wv, wo, wg, wu, wd, gain_a, gain_m, cos, sin, y,
           own, precv, psend, b, held, rbuf, sbuf, ring, ring_d, hid, xv, av, qv, kv, vv, seen,
           ssem, rsem, xssem, xrsem, dssem, drsem1, drsem2, lsem, gsem, dsem, xsem, credit):
    d_model = x.shape[1]
    ng, nd, nw = wg.shape[1] // 256, d_model // 512, d_model // 1024
    wide = 1024
    z, c = lax.axis_index("tp") // 2, lax.axis_index("tp") % 2
    dp = lax.axis_index("dp")

    def device(chip, core):
        return dp, chip * 2 + core

    partner = device(z, 1 - c)

    def remote(src, dst, send, recv, target):
        return pltpu.make_async_remote_copy(src_ref=src, dst_ref=dst, send_sem=send, recv_sem=recv, device_id=target, device_id_type=MESH)

    def rows_of(n):
        return pl.ds(pl.multiple_of(n, ROWS), ROWS)

    def service(d, s):
        p = z if d == 0 else CHIPS - 1 - z
        i = s - HOP * p
        nxt = device(z + 1 if d == 0 else z - 1, c)

        @pl.when((i >= 0) & (i < NJ))
        def _():
            job, sub = i // PIECES, i % PIECES
            code = pick(job, [t * K + k for t, k in JOBS])
            t, k = code // K, code % K
            q = i % 8
            send, recv = ssem.at[d, q], rsem.at[d, q]

            @pl.when(p > 0)
            def _():
                remote(rbuf.at[d, q], rbuf.at[d, q], send, recv, nxt).wait_recv()

            @pl.when((p < CHIPS - 1) & (i >= 4))
            def _():
                remote(sbuf.at[d, 0], rbuf.at[d, q], ssem.at[d, (i + 4) % 8], recv, nxt).wait_send()

            def reduce(a):
                sl = k % 2
                at = rows_of(d * QUARTER + sub * ROWS)
                mine = rows_of(sub * ROWS)
                early = z < 2 if d == 0 else z >= 2

                @pl.when((sub == 0) & early)
                def _():
                    remote(psend.at[a], precv.at[a, sl], xssem.at[a], xrsem.at[a, sl], partner).wait_recv()

                def total(cols, first):
                    v = own[a, sl, at, cols] + precv[a, sl, at, cols].astype(jnp.float32)
                    return v if first else v + rbuf[d, q, :, cols].astype(jnp.float32)

                for first in (True, False):
                    @pl.when((p == 0) if first else (p > 0) & (p < CHIPS - 1))
                    def _():
                        for j in range(0, d_model, wide):
                            cols = pl.ds(j, wide)
                            sbuf[d, i % 4, :, cols] = total(cols, first).astype(jnp.bfloat16)

                @pl.when(p < CHIPS - 1)
                def _():
                    remote(sbuf.at[d, i % 4], rbuf.at[d, q], send, recv, nxt).start()

                @pl.when(p == CHIPS - 1)
                def _():
                    if a == 0:
                        squares = jnp.zeros((ROWS, 128), jnp.float32)
                        for j in range(0, d_model, wide):
                            cols = pl.ds(j, wide)
                            h = total(cols, False).astype(jnp.bfloat16)
                            held[k, mine, cols] = h
                            h = h.astype(jnp.float32)
                            h *= h
                            for n in range(0, wide, 128):
                                squares += h[:, n : n + 128]
                        scale = lax.rsqrt(jnp.sum(squares, -1, keepdims=True) * (1 / d_model) + 1e-6)
                        for j in range(0, d_model, wide):
                            cols = pl.ds(j, wide)
                            h = held[k, mine, cols].astype(jnp.float32)
                            b[k % NB, at, cols] = (h * scale * gain_m[:, cols]).astype(jnp.bfloat16)
                    else:
                        for j in range(0, d_model, wide):
                            cols = pl.ds(j, wide)
                            held[k, mine, cols] = (held[k, mine, cols].astype(jnp.float32) + total(cols, False)).astype(jnp.bfloat16)

                @pl.when((sub == PIECES - 1) & jnp.logical_not(early) & (k + 2 < K))
                def _():
                    pl.semaphore_signal(credit.at[a], inc=1, device_id=partner, device_id_type=MESH)

            def spread_sum(a):
                at = (1 - d) * QUARTER + sub * ROWS
                ds = dssem.at[a, d, k % 2, sub]
                if a == 0:
                    here, there = b.at[k % NB, rows_of(at)], b.at[k % NB, rows_of(HALF + at)]
                    dr = drsem1.at[k % NB]
                else:
                    here = there = y.at[rows_of(k * T + c * HALF + at)]
                    dr = drsem2.at[k]

                @pl.when(k >= 2)
                def _():
                    remote(sbuf.at[d, 0], rbuf.at[d, q], ds, recv, partner).wait_send()

                def go(src):
                    @pl.when(p < CHIPS - 1)
                    def _():
                        remote(src, here, send, recv, nxt).start()

                    remote(src, there, ds, dr, partner).start()

                if a == 0:
                    go(here)
                else:
                    @pl.when(p > 0)
                    def _():
                        go(here)

                    @pl.when(p == 0)
                    def _():
                        src = held.at[k, rows_of(sub * ROWS)]
                        go(src)

                        @pl.when(k >= 2)
                        def _():
                            pltpu.make_async_copy(src, here, lsem.at[k % 2, sub]).wait()

                        pltpu.make_async_copy(src, here, lsem.at[k % 2, sub]).start()

            pl.when(t == R1)(lambda: reduce(0))
            pl.when(t == A1)(lambda: spread_sum(0))
            pl.when(t == R2)(lambda: reduce(1))
            pl.when(t == A2)(lambda: spread_sum(1))

    def slots(s, n):
        def one(m, _):
            service(0, s + m)
            service(1, s + m)
            return 0

        lax.fori_loop(0, n, one, 0)

    def exchange(a, k):
        @pl.when(k >= 2)
        def _():
            pl.semaphore_wait(credit.at[a], 1)

        remote(psend.at[a], precv.at[a, k % 2], xssem.at[a], xrsem.at[a, k % 2], partner).start()

    def exchanged(a, k):
        @pl.when(k >= 1)
        def _():
            remote(psend.at[a], precv.at[a, k % 2], xssem.at[a], xrsem.at[a, k % 2], partner).wait_send()

    def copies_q(sl):
        return [pltpu.make_async_copy(wq, ring.at[sl], gsem.at[sl, 0])]

    def copies_kv(sl):
        return [pltpu.make_async_copy(w, ring.at[sl, :, pl.ds(n * 128, 128)], gsem.at[sl, n]) for n, w in enumerate((wk, wv))]

    def copies_gu(sl, j):
        cols = pl.ds(pl.multiple_of(j * 256, 256), 256)
        return [pltpu.make_async_copy(w.at[:, cols], ring.at[sl, :, pl.ds(n * 256, 256)], gsem.at[sl, n]) for n, w in enumerate((wg, wu))]

    def copies_d(sl, j):
        return [pltpu.make_async_copy(wd.at[:, pl.ds(pl.multiple_of(j * 512, 512), 512)], ring_d.at[sl], dsem.at[sl, 0])]

    def copies_o(sl, j):
        return [pltpu.make_async_copy(wo.at[:, pl.ds(pl.multiple_of(j * 1024 + n * 512, 512), 512)], ring_d.at[sl, pl.ds(n * HEAD * 4, HEAD * 4)],
                                      dsem.at[sl, n]) for n in range(2)]

    def start(copies):
        for copy in copies:
            copy.start()

    def wait(copies):
        for copy in copies:
            copy.wait()

    last = K + LEAD - 1

    def ring_place(it, pos):
        return pos + jnp.where(it < LEAD, 2 * it, jnp.where(it < K, 2 * LEAD + (ng + 2) * (it - LEAD), 2 * LEAD + (ng + 2) * (K - LEAD) + ng * (it - K)))

    def ring_d_place(it, pos):
        return pos + jnp.where(it < LEAD, nw * it, jnp.where(it < K, nw * LEAD + (nd + nw) * (it - LEAD), nw * LEAD + (nd + nw) * (K - LEAD) + nd * (it - K)))

    def next_round(it, sl, pos, has_mlp, has_att, mlp, att):
        nxt = it + 1
        if has_mlp:
            pl.when((nxt >= LEAD) & (nxt <= last))(lambda: start(mlp(sl, pos)))
        if has_att:
            pl.when(nxt < LEAD)(lambda: start(att(sl, pos)))

    def attn_load(sl, pos):
        return copies_q(sl) if pos == 0 else copies_kv(sl)

    def x_copy(k):
        return pltpu.make_async_copy(x.at[pl.ds(pl.multiple_of(k * T, T), T)], xv, xsem)

    def norm(k):
        x_copy(k).wait()

        def some(r, _):
            at = pl.ds(pl.multiple_of(r * ROWS, ROWS), ROWS)
            squares = jnp.zeros((ROWS, 128), jnp.float32)
            for j in range(0, d_model, wide):
                v = xv[at, pl.ds(j, wide)].astype(jnp.float32)
                v *= v
                for n in range(0, wide, 128):
                    squares += v[:, n : n + 128]
            scale = lax.rsqrt(jnp.sum(squares, -1, keepdims=True) * (1 / d_model) + 1e-6)
            for j in range(0, d_model, wide):
                cols = pl.ds(j, wide)
                av[at, cols] = (xv[at, cols].astype(jnp.float32) * scale * gain_a[:, cols]).astype(jnp.bfloat16)
            return 0

        lax.fori_loop(0, T // ROWS, some, 0)

    def turned(t, at):
        t = t.astype(jnp.bfloat16).astype(jnp.float32)
        return (t * cos[at, :] + pltpu.roll(t, HEAD // 2, 1) * sin[at, :]).astype(jnp.bfloat16)

    def project_q(it):
        k = it
        pos = jnp.where(it < LEAD, 0, ng)
        sl = ring_place(it, pos) % 2
        wait(copies_q(sl))
        at = pl.ds(pl.multiple_of((k % 2) * T, T), T)
        out = jnp.dot(av[...], ring[sl], preferred_element_type=jnp.float32)
        for n in range(4):
            qv[n] = turned(out[:, n * HEAD : (n + 1) * HEAD], at)
        pl.when(it < LEAD - 1)(lambda: start(copies_q(sl)))
        pl.when(it >= LEAD - 1)(lambda: start(copies_gu(sl, 0)))

    def project_kv(it):
        k = it
        pos = jnp.where(it < LEAD, 1, ng + 1)
        sl = ring_place(it, pos) % 2
        wait(copies_kv(sl))
        at = pl.ds(pl.multiple_of((k % 2) * T, T), T)
        out = jnp.dot(av[...], ring[sl, :, :256], preferred_element_type=jnp.float32)
        kv[at, :] = turned(out[:, :HEAD], at)
        vv[at, :] = out[:, HEAD:].astype(jnp.bfloat16)
        pl.when(it < LEAD - 1)(lambda: start(copies_kv(sl)))
        pl.when(it >= LEAD - 1)(lambda: start(copies_gu(sl, 1)))

    def attend(k, heads):
        scale = HEAD**-0.5
        hidden = lax.broadcasted_iota(jnp.int32, (T, T), 1) > lax.broadcasted_iota(jnp.int32, (T, T), 0)

        def work(n, both):
            def scores(at):
                return lax.dot_general(qv[n], kv[at, :], (((1,), (1,)), ((), ())), preferred_element_type=jnp.float32) * scale

            here = pl.ds(T, T) if both else pl.ds(0, T)
            parts = [(jnp.where(hidden, -1e30, scores(here)), here)]
            if both:
                parts.append((scores(pl.ds(0, T)), pl.ds(0, T)))
            top = functools.reduce(jnp.maximum, [s.max(-1, keepdims=True) for s, _ in parts])
            out, total = 0.0, 0.0
            for s, at in parts:
                w = jnp.exp(s - top)
                total += w.sum(-1, keepdims=True)
                out += jnp.dot(w.astype(jnp.bfloat16), vv[at, :], preferred_element_type=jnp.float32)
            out = (out / total).astype(jnp.bfloat16)
            cols = pl.ds(pl.multiple_of(n * HEAD, HEAD), HEAD)
            seen[pl.ds(pl.multiple_of(c * HALF, HALF), HALF), cols] = out[:HALF]
            seen[pl.ds(pl.multiple_of((1 - c) * HALF, HALF), HALF), cols] = out[HALF:]

        for both in (False, True):
            @pl.when((k % 2 == 1) if both else (k % 2 == 0))
            def _():
                def one(n, _):
                    work(n, both)
                    return 0

                lax.fori_loop(heads[0], heads[1], one, 0)

    def give(a, sl, cols, out):
        own[a, sl, :, cols] = out[:HALF]
        psend[a, :, cols] = out[HALF:].astype(jnp.bfloat16)

    def out_project(it, j):
        k = it
        pos = jnp.where(it < LEAD, 0, nd) + j
        sl = ring_d_place(it, pos) % 2
        pl.when(j == 0)(lambda: exchanged(0, k))
        wait(copies_o(sl, j))
        for n in range(2):
            out = jnp.dot(seen[...], ring_d[sl, pl.ds(n * HEAD * 4, HEAD * 4), :], preferred_element_type=jnp.float32)
            give(0, k % 2, pl.ds(pl.multiple_of(j * 1024 + n * 512, 512), 512), out)
        pl.when(j < nw - 2)(lambda: start(copies_o(sl, j + 2)))
        pl.when((j >= nw - 2) & (it < LEAD - 1))(lambda: start(copies_o(sl, j + 2 - nw)))
        pl.when((j >= nw - 2) & (it >= LEAD - 1))(lambda: start(copies_d(sl, j + 2 - nw)))

        @pl.when(j == nw - 1)
        def _():
            for chip, d in ((CHIPS - 1, 0), (0, 1)):
                @pl.when(z == chip)
                def _():
                    def some(r, _):
                        at = rows_of(d * QUARTER + r * ROWS)
                        from_x = rows_of(c * HALF + d * QUARTER + r * ROWS)
                        for jj in range(0, d_model, wide):
                            cols = pl.ds(jj, wide)
                            own[0, k % 2, at, cols] += xv[from_x, cols].astype(jnp.float32)
                        return 0

                    lax.fori_loop(0, PIECES, some, 0)

            exchange(0, k)
            pl.when(k + 1 < K)(lambda: x_copy(k + 1).start())

    def gate_up(it, j):
        k = it - LEAD
        sl = ring_place(it, j) % 2

        @pl.when(j == 0)
        def _():
            remote(b.at[k % NB, pl.ds(0, HALF)], b.at[k % NB, pl.ds(HALF, HALF)], xssem.at[0], drsem1.at[k % NB], partner).wait_recv()

        wait(copies_gu(sl, j))
        out = jnp.dot(b[k % NB], ring[sl], preferred_element_type=jnp.float32)
        hid[:, pl.ds(pl.multiple_of(j * 256, 256), 256)] = (jax.nn.silu(out[:, :256]) * out[:, 256:]).astype(jnp.bfloat16)
        pl.when(j < ng - 2)(lambda: start(copies_gu(sl, j + 2)))
        pl.when((j == ng - 2) & (it < K))(lambda: start(copies_q(sl)))
        pl.when((j == ng - 1) & (it < K))(lambda: start(copies_kv(sl)))
        pl.when((j >= ng - 2) & (it >= K) & (it < last))(lambda: start(copies_gu(sl, j + 2 - ng)))

    def down(it, j):
        k = it - LEAD
        sl = ring_d_place(it, j) % 2
        pl.when(j == 0)(lambda: exchanged(1, k))
        wait(copies_d(sl, j))
        out = jnp.dot(hid[...], ring_d[sl], preferred_element_type=jnp.float32)
        give(1, k % 2, pl.ds(pl.multiple_of(j * 512, 512), 512), out)
        pl.when(j < nd - 2)(lambda: start(copies_d(sl, j + 2)))
        pl.when((j >= nd - 2) & (it < K))(lambda: start(copies_o(sl, j + 2 - nd)))
        pl.when((j >= nd - 2) & (it >= K) & (it < last))(lambda: start(copies_d(sl, j + 2 - nd)))
        pl.when(j == nd - 1)(lambda: exchange(1, k))

    x_copy(0).start()
    start(copies_q(0))
    start(copies_kv(1))
    start(copies_o(0, 0))
    start(copies_o(1, 1))

    barrier = pltpu.get_barrier_semaphore()
    for there, who in ((z < CHIPS - 1, device(z + 1, c)), (z > 0, device(z - 1, c)), (z >= 0, partner)):
        pl.when(there)(functools.partial(pl.semaphore_signal, barrier, inc=1, device_id=who, device_id_type=MESH))
    pl.semaphore_wait(barrier, jnp.where((z > 0) & (z < CHIPS - 1), 3, 2))

    first_att = ng + nd
    units = first_att + 5 + nw
    after = np.zeros((K + LEAD, units), int)
    for it in range(K + LEAD):
        if it >= LEAD:
            busy = it < K
            after[it, :ng] = spread(7 if busy else 5, ng)
            after[it, ng:first_att] = spread(2 if busy else 3, nd)
        if it < K:
            tail = after[it, first_att:]
            tail[:5] = {0: (0, 0, 0, 0, 0), 1: (1, 1, 0, 1, 1), 2: (1, 1, 1, 1, 2), 3: (1, 1, 0, 1, 1)}.get(it, (1, 1, 1, 1, 1))
            if it == 3:
                tail[-1] = 4
    kinds = [0, 1, 2, 3] + [LEAD] * (K - LEAD) + [LEAD + 1] * LEAD
    tables = [list(after[kinds.index(n)]) for n in range(LEAD + 2)]
    assert all(list(after[it]) == tables[kinds[it]] for it in range(K + LEAD))

    def round_(it, s):
        kind = pick(it, kinds)

        def unit(u, s):
            pl.when(u < ng)(lambda: gate_up(it, u))
            pl.when((u >= ng) & (u < first_att))(lambda: down(it, u - ng))
            pl.when(u == first_att)(lambda: norm(it))
            pl.when(u == first_att + 1)(lambda: project_q(it))
            pl.when(u == first_att + 2)(lambda: project_kv(it))
            pl.when((u == first_att + 3) | (u == first_att + 4))(lambda: attend(it, (2 * (u - first_att - 3), 2 * (u - first_att - 3) + 2)))
            pl.when((u >= first_att + 5) & (u < units))(lambda: out_project(it, u - first_att - 5))
            n = pick(kind * units + u, [n for table in tables for n in table])
            n = jnp.where(it > last, NS - s, n)
            slots(s, n)
            return s + n

        low = jnp.where(it < LEAD, first_att, 0)
        high = jnp.where(it < K, units, first_att)
        low, high = jnp.where(it > last, units, low), jnp.where(it > last, units + 1, high)
        return lax.fori_loop(low, high, unit, s)

    lax.fori_loop(0, K + LEAD + 1, round_, jnp.int32(0))

    for d in range(2):
        p = z if d == 0 else CHIPS - 1 - z

        @pl.when(p < CHIPS - 1)
        def _():
            for i in range(NJ - 4, NJ):
                remote(sbuf.at[d, 0], rbuf.at[d, 0], ssem.at[d, i % 8], rsem.at[d, 0], partner).wait_send()

        for a in range(2):
            for k in (K - 2, K - 1):
                for sub in range(PIECES):
                    remote(sbuf.at[d, 0], rbuf.at[d, 0], dssem.at[a, d, k % 2, sub], rsem.at[d, 0], partner).wait_send()

        @pl.when(p == 0)
        def _():
            for k in (K - 2, K - 1):
                for sub in range(PIECES):
                    pltpu.make_async_copy(held.at[k, rows_of(sub * ROWS)], y.at[rows_of(0)], lsem.at[k % 2, sub]).wait()

    for a in range(2):
        exchanged(a, K)
    for k in range(K):
        remote(y.at[pl.ds(0, HALF)], y.at[pl.ds(0, HALF)], xssem.at[0], drsem2.at[k], partner).wait_recv()


def layer(x, gain_a, wq, wk, wv, wo, gain_m, w_gate, w_up, w_down):
    batch, rows, d = x.shape
    ff = w_gate.shape[1]
    bf, f32 = jnp.bfloat16, jnp.float32
    half = HEAD // 2
    angle = np.arange(rows, dtype=np.float32)[:, None] * np.power(np.float32(THETA), -np.arange(half, dtype=np.float32) / np.float32(half))
    angle = angle.astype(np.float64)
    cos = jnp.asarray(np.concatenate([np.cos(angle), np.cos(angle)], -1), f32)
    sin = jnp.asarray(np.concatenate([-np.sin(angle), np.sin(angle)], -1), f32)
    dma, reg = pltpu.SemaphoreType.DMA, pltpu.SemaphoreType.REGULAR
    anywhere, near = pl.BlockSpec(memory_space=pl.ANY), pl.BlockSpec(memory_space=pltpu.VMEM)
    tokens = batch * rows
    flops = 2 * tokens * (d * (wq.shape[1] * 2 + wk.shape[1] * 2 + 3 * ff) + rows * wq.shape[1])
    out = pl.pallas_call(
        kernel,
        out_shape=jax.ShapeDtypeStruct((tokens, d), bf),
        in_specs=[anywhere] * 8 + [near] * 4,
        out_specs=anywhere,
        scratch_shapes=[
            pltpu.VMEM((2, 2, HALF, d), f32),
            pltpu.VMEM((2, 2, HALF, d), bf),
            pltpu.VMEM((2, HALF, d), bf),
            pltpu.VMEM((NB, T, d), bf),
            pltpu.VMEM((K, QUARTER, d), bf),
            pltpu.VMEM((2, 8, ROWS, d), bf),
            pltpu.VMEM((2, 4, ROWS, d), bf),
            pltpu.VMEM((2, d, 512), bf),
            pltpu.VMEM((2, ff, 512), bf),
            pltpu.VMEM((T, ff), bf),
            pltpu.VMEM((T, d), bf),
            pltpu.VMEM((T, d), bf),
            pltpu.VMEM((4, T, HEAD), bf),
            pltpu.VMEM((2 * T, HEAD), bf),
            pltpu.VMEM((2 * T, HEAD), bf),
            pltpu.VMEM((T, 4 * HEAD), bf),
            dma((2, 8)), dma((2, 8)),
            dma((2,)), dma((2, 2)),
            dma((2, 2, 2, PIECES)), dma((NB,)), dma((K,)), dma((2, PIECES)),
            dma((2, 2)), dma((2, 2)), dma,
            reg((2,)),
        ],
        compiler_params=pltpu.CompilerParams(collective_id=0, has_side_effects=True, vmem_limit_bytes=VMEM),
        cost_estimate=pl.CostEstimate(flops=flops, bytes_accessed=8 * tokens * d, transcendentals=0),
    )(x.reshape(tokens, d), wq, wk, wv, wo, w_gate, w_up, w_down, gain_a.astype(f32).reshape(1, d), gain_m.astype(f32).reshape(1, d), cos, sin)
    return out.reshape(x.shape)


def solution(mesh):
    tokens, whole, columns, rows_of = P("dp", None, None), P(None), P(None, "tp"), P("tp", None)
    return jax.shard_map(
        layer,
        mesh=mesh,
        in_specs=(tokens, whole, columns, columns, columns, rows_of, whole, columns, columns, rows_of),
        out_specs=tokens,
        check_vma=False,
    )
```

```python
import functools

import jax
import jax.numpy as jnp
import numpy as np
from jax import lax
from jax.experimental import pallas as pl
from jax.experimental.pallas import tpu as pltpu
from jax.sharding import PartitionSpec as P

HEAD = 128
THETA = 10000
MESH = pl.DeviceIdType.MESH
CHIPS = 4
T = 256
HALF = T // 2
QUARTER = T // 4
PIECES = 4
ROWS = QUARTER // PIECES
HOP = 2
K = 8
LEAD = 4
R1, A1, R2, A2 = range(4)
JOBS = [(R1, 0), (R1, 1), (A1, 0), (R1, 2), (A1, 1), (A1, 2), (R1, 3), (R2, 0), (R1, 4), (A1, 3), (R2, 1), (A1, 4), (R1, 5), (A2,
        1), (R2, 2), (R1, 6), (A2, 0), (A1, 5), (R2, 3), (R1, 7), (A1, 6), (R2, 4), (A1, 7), (A2, 2), (R2, 5), (A2, 4), (A2, 3), (R2, 6),
        (A2, 5), (R2, 7), (A2, 6), (A2, 7)]
SLOTS = [(0, 0), (5,), (5, 2), (4, 2), (13,), (14,), (14,), (14,), (11,), (10,), (11,), (12,)]
NJ = len(JOBS) * PIECES
NS = NJ + HOP * (CHIPS - 1)
NB = 3
VMEM = 67_043_328


def pick(index, table):
    out = jnp.int32(0)
    for n, value in enumerate(table):
        if value:
            out += jnp.where(index == n, jnp.int32(value), jnp.int32(0))
    return out


def spread(total, count):
    return [total * (n + 1) // count - total * n // count for n in range(count)]


def kernel(x, wq, wk, wv, wo, wg, wu, wd, gains_a, gains_m, turns, y,
           own, precv, psend, b, held, rbuf, sbuf, ring, ring_d, hid, xv, av, qv, kv, vv, seen, raw, gain_a, gain_m, cos_sin,
           ssem, rsem, xssem, xrsem, dssem, drsem1, drsem2, lsem, gsem, dsem, xsem, csem, credit):
    d_model = x.shape[1]
    cos, sin = cos_sin.at[0], cos_sin.at[1]
    ng, nd, nw = wg.shape[1] // 256, d_model // 512, d_model // 1024
    wide = 1024
    z, c = lax.axis_index("tp") // 2, lax.axis_index("tp") % 2
    dp = lax.axis_index("dp")

    def device(chip, core):
        return dp, chip * 2 + core

    partner = device(z, 1 - c)

    def remote(src, dst, send, recv, target):
        return pltpu.make_async_remote_copy(src_ref=src, dst_ref=dst, send_sem=send, recv_sem=recv, device_id=target, device_id_type=MESH)

    def rows_of(n):
        return pl.ds(pl.multiple_of(n, ROWS), ROWS)

    def service(d, s):
        p = z if d == 0 else CHIPS - 1 - z
        i = s - HOP * p
        nxt = device(z + 1 if d == 0 else z - 1, c)

        @pl.when((i >= 0) & (i < NJ))
        def _():
            job, sub = i // PIECES, i % PIECES
            code = pick(job, [t * K + k for t, k in JOBS])
            t, k = code // K, code % K
            q = i % 8
            send, recv = ssem.at[d, q], rsem.at[d, q]

            @pl.when(p > 0)
            def _():
                remote(rbuf.at[d, q], rbuf.at[d, q], send, recv, nxt).wait_recv()

            @pl.when((p < CHIPS - 1) & (i >= 4))
            def _():
                remote(sbuf.at[d, 0], rbuf.at[d, q], ssem.at[d, (i + 4) % 8], recv, nxt).wait_send()

            def reduce(a):
                sl = k % 2
                at = rows_of(d * QUARTER + sub * ROWS)
                mine = rows_of(sub * ROWS)
                early = z < 2 if d == 0 else z >= 2

                @pl.when((sub == 0) & early)
                def _():
                    remote(psend.at[a], precv.at[a, sl], xssem.at[a], xrsem.at[a, sl], partner).wait_recv()

                def total(cols, first):
                    v = own[a, sl, at, cols] + precv[a, sl, at, cols].astype(jnp.float32)
                    return v if first else v + rbuf[d, q, :, cols].astype(jnp.float32)

                for first in (True, False):
                    @pl.when((p == 0) if first else (p > 0) & (p < CHIPS - 1))
                    def _():
                        for j in range(0, d_model, wide):
                            cols = pl.ds(j, wide)
                            sbuf[d, i % 4, :, cols] = total(cols, first).astype(jnp.bfloat16)

                @pl.when(p < CHIPS - 1)
                def _():
                    remote(sbuf.at[d, i % 4], rbuf.at[d, q], send, recv, nxt).start()

                @pl.when(p == CHIPS - 1)
                def _():
                    if a == 0:
                        squares = jnp.zeros((ROWS, 128), jnp.float32)
                        for j in range(0, d_model, wide):
                            cols = pl.ds(j, wide)
                            h = total(cols, False).astype(jnp.bfloat16)
                            held[k, mine, cols] = h
                            h = h.astype(jnp.float32)
                            h *= h
                            for n in range(0, wide, 128):
                                squares += h[:, n : n + 128]
                        scale = lax.rsqrt(jnp.sum(squares, -1, keepdims=True) * (1 / d_model) + 1e-6)
                        for j in range(0, d_model, wide):
                            cols = pl.ds(j, wide)
                            h = held[k, mine, cols].astype(jnp.float32)
                            b[k % NB, at, cols] = (h * scale * gain_m[:, cols]).astype(jnp.bfloat16)
                    else:
                        for j in range(0, d_model, wide):
                            cols = pl.ds(j, wide)
                            held[k, mine, cols] = (held[k, mine, cols].astype(jnp.float32) + total(cols, False)).astype(jnp.bfloat16)

                @pl.when((sub == PIECES - 1) & jnp.logical_not(early) & (k + 2 < K))
                def _():
                    pl.semaphore_signal(credit.at[a], inc=1, device_id=partner, device_id_type=MESH)

            def spread_sum(a):
                at = (1 - d) * QUARTER + sub * ROWS
                ds = dssem.at[a, d, k % NB if a == 0 else k % 2, sub]
                if a == 0:
                    here, there = b.at[k % NB, rows_of(at)], b.at[k % NB, rows_of(HALF + at)]
                    dr = drsem1.at[k % NB]
                else:
                    here = there = y.at[rows_of(k * T + c * HALF + at)]
                    dr = drsem2.at[k]

                if a == 1:
                    pl.when(k >= 2)(remote(sbuf.at[d, 0], rbuf.at[d, q], ds, recv, partner).wait_send)

                def go(src):
                    @pl.when(p < CHIPS - 1)
                    def _():
                        remote(src, here, send, recv, nxt).start()

                    remote(src, there, ds, dr, partner).start()

                if a == 0:
                    go(here)
                else:
                    @pl.when(p > 0)
                    def _():
                        go(here)

                    @pl.when(p == 0)
                    def _():
                        src = held.at[k, rows_of(sub * ROWS)]
                        go(src)

                        @pl.when(k >= 2)
                        def _():
                            pltpu.make_async_copy(src, here, lsem.at[k % 2, sub]).wait()

                        pltpu.make_async_copy(src, here, lsem.at[k % 2, sub]).start()

            pl.when(t == R1)(lambda: reduce(0))
            pl.when(t == A1)(lambda: spread_sum(0))
            pl.when(t == R2)(lambda: reduce(1))
            pl.when(t == A2)(lambda: spread_sum(1))

    def slots(s, n):
        def one(m, _):
            service(0, s + m)
            service(1, s + m)
            return 0

        lax.fori_loop(0, n, one, 0)

    def exchange(a, k):
        @pl.when(k >= 2)
        def _():
            pl.semaphore_wait(credit.at[a], 1)

        remote(psend.at[a], precv.at[a, k % 2], xssem.at[a], xrsem.at[a, k % 2], partner).start()

    def exchanged(a, k):
        @pl.when(k >= 1)
        def _():
            remote(psend.at[a], precv.at[a, k % 2], xssem.at[a], xrsem.at[a, k % 2], partner).wait_send()

    def copies_q(sl):
        return [pltpu.make_async_copy(wq, ring.at[sl], gsem.at[sl, 0])]

    def copies_kv(sl):
        return [pltpu.make_async_copy(w, ring.at[sl, :, pl.ds(n * 128, 128)], gsem.at[sl, n]) for n, w in enumerate((wk, wv))]

    def copies_gu(sl, j):
        cols = pl.ds(pl.multiple_of(j * 256, 256), 256)
        return [pltpu.make_async_copy(w.at[:, cols], ring.at[sl, :, pl.ds(n * 256, 256)], gsem.at[sl, n]) for n, w in enumerate((wg, wu))]

    def copies_d(sl, j):
        return [pltpu.make_async_copy(wd.at[:, pl.ds(pl.multiple_of(j * 512, 512), 512)], ring_d.at[sl], dsem.at[sl, 0])]

    def copies_o(sl, j):
        return [pltpu.make_async_copy(wo.at[:, pl.ds(pl.multiple_of(j * 1024 + n * 512, 512), 512)], ring_d.at[sl, pl.ds(n * HEAD * 4, HEAD * 4)],
                                      dsem.at[sl, n]) for n in range(2)]

    def start(copies):
        for copy in copies:
            copy.start()

    def wait(copies):
        for copy in copies:
            copy.wait()

    last = K + LEAD - 1

    def ring_place(it, pos):
        return pos + jnp.where(it < LEAD, 2 * it, jnp.where(it < K, 2 * LEAD + (ng + 2) * (it - LEAD), 2 * LEAD + (ng + 2) * (K - LEAD) + ng * (it - K)))

    def ring_d_place(it, pos):
        return pos + jnp.where(it < LEAD, nw * it, jnp.where(it < K, nw * LEAD + (nd + nw) * (it - LEAD), nw * LEAD + (nd + nw) * (K - LEAD) + nd * (it - K)))

    def next_round(it, sl, pos, has_mlp, has_att, mlp, att):
        nxt = it + 1
        if has_mlp:
            pl.when((nxt >= LEAD) & (nxt <= last))(lambda: start(mlp(sl, pos)))
        if has_att:
            pl.when(nxt < LEAD)(lambda: start(att(sl, pos)))

    def attn_load(sl, pos):
        return copies_q(sl) if pos == 0 else copies_kv(sl)

    def x_copy(k):
        return pltpu.make_async_copy(x.at[pl.ds(pl.multiple_of(k * T, T), T)], xv, xsem)

    def norm(k, quarters):
        pl.when(quarters[0] == 0)(x_copy(k).wait)

        def some(r, _):
            at = pl.ds(pl.multiple_of(r * QUARTER, QUARTER), QUARTER)
            squares = jnp.zeros((QUARTER, 128), jnp.float32)
            for j in range(0, d_model, 256):
                v = xv[at, pl.ds(j, 256)].astype(jnp.float32)
                v *= v
                squares += v[:, :128] + v[:, 128:]
            scale = lax.rsqrt(jnp.sum(squares, -1, keepdims=True) * (1 / d_model) + 1e-6)
            for j in range(0, d_model, 256):
                cols = pl.ds(j, 256)
                av[at, cols] = (xv[at, cols].astype(jnp.float32) * scale * gain_a[:, cols]).astype(jnp.bfloat16)
            return 0

        lax.fori_loop(quarters[0], quarters[1], some, 0)

    def turned(t, at):
        t = t.astype(jnp.bfloat16).astype(jnp.float32)
        return (t * cos[at, :] + pltpu.roll(t, HEAD // 2, 1) * sin[at, :]).astype(jnp.bfloat16)

    def project_q(it):
        k = it
        pos = jnp.where(it < LEAD, 0, ng)
        sl = ring_place(it, pos) % 2
        wait(copies_q(sl))
        at = pl.ds(pl.multiple_of((k % 2) * T, T), T)
        out = jnp.dot(av[...], ring[sl], preferred_element_type=jnp.float32)
        for n in range(4):
            qv[n] = turned(out[:, n * HEAD : (n + 1) * HEAD], at)
        pl.when(it < LEAD - 1)(lambda: start(copies_q(sl)))
        pl.when(it >= LEAD - 1)(lambda: start(copies_gu(sl, 0)))

    def project_kv(it):
        k = it
        pos = jnp.where(it < LEAD, 1, ng + 1)
        sl = ring_place(it, pos) % 2
        wait(copies_kv(sl))
        at = pl.ds(pl.multiple_of((k % 2) * T, T), T)
        out = jnp.dot(av[...], ring[sl, :, :256], preferred_element_type=jnp.float32)
        kv[at, :] = turned(out[:, :HEAD], at)
        vv[at, :] = out[:, HEAD:].astype(jnp.bfloat16)
        pl.when(it < LEAD - 1)(lambda: start(copies_kv(sl)))
        pl.when(it >= LEAD - 1)(lambda: start(copies_gu(sl, 1)))

    def attend(k, heads):
        scale = HEAD**-0.5
        hidden = lax.broadcasted_iota(jnp.int32, (T, T), 1) > lax.broadcasted_iota(jnp.int32, (T, T), 0)

        def work(n, both):
            def scores(at):
                return lax.dot_general(qv[n], kv[at, :], (((1,), (1,)), ((), ())), preferred_element_type=jnp.float32) * scale

            here = pl.ds(T, T) if both else pl.ds(0, T)
            parts = [(jnp.where(hidden, -1e30, scores(here)), here)]
            if both:
                parts.append((scores(pl.ds(0, T)), pl.ds(0, T)))
            top = functools.reduce(jnp.maximum, [s.max(-1, keepdims=True) for s, _ in parts])
            out, total = 0.0, 0.0
            for s, at in parts:
                w = jnp.exp(s - top)
                total += w.sum(-1, keepdims=True)
                out += jnp.dot(w.astype(jnp.bfloat16), vv[at, :], preferred_element_type=jnp.float32)
            out = (out / total).astype(jnp.bfloat16)
            cols = pl.ds(pl.multiple_of(n * HEAD, HEAD), HEAD)
            seen[pl.ds(pl.multiple_of(c * HALF, HALF), HALF), cols] = out[:HALF]
            seen[pl.ds(pl.multiple_of((1 - c) * HALF, HALF), HALF), cols] = out[HALF:]

        for both in (False, True):
            @pl.when((k % 2 == 1) if both else (k % 2 == 0))
            def _():
                def one(n, _):
                    work(n, both)
                    return 0

                lax.fori_loop(heads[0], heads[1], one, 0)

    def give(a, sl, cols, out):
        own[a, sl, :, cols] = out[:HALF]
        psend[a, :, cols] = out[HALF:].astype(jnp.bfloat16)

    def out_project(it, j):
        k = it
        pos = jnp.where(it < LEAD, 0, nd) + j
        sl = ring_d_place(it, pos) % 2
        pl.when(j == 0)(lambda: exchanged(0, k))
        wait(copies_o(sl, j))
        for n in range(2):
            out = jnp.dot(seen[...], ring_d[sl, pl.ds(n * HEAD * 4, HEAD * 4), :], preferred_element_type=jnp.float32)
            give(0, k % 2, pl.ds(pl.multiple_of(j * 1024 + n * 512, 512), 512), out)
        pl.when(j < nw - 2)(lambda: start(copies_o(sl, j + 2)))
        pl.when((j >= nw - 2) & (it < LEAD - 1))(lambda: start(copies_o(sl, j + 2 - nw)))
        pl.when((j >= nw - 2) & (it >= LEAD - 1))(lambda: start(copies_d(sl, j + 2 - nw)))

        @pl.when(j == nw - 1)
        def _():
            for chip, d in ((CHIPS - 1, 0), (0, 1)):
                @pl.when(z == chip)
                def _():
                    def some(r, _):
                        at = rows_of(d * QUARTER + r * ROWS)
                        from_x = rows_of(c * HALF + d * QUARTER + r * ROWS)
                        for jj in range(0, d_model, wide):
                            cols = pl.ds(jj, wide)
                            own[0, k % 2, at, cols] += xv[from_x, cols].astype(jnp.float32)
                        return 0

                    lax.fori_loop(0, PIECES, some, 0)

            exchange(0, k)
            pl.when(k + 1 < K)(lambda: x_copy(k + 1).start())

    def gate_up(it, j):
        k = it - LEAD
        sl = ring_place(it, j) % 2

        @pl.when(j == 0)
        def _():
            remote(b.at[k % NB, pl.ds(0, HALF)], b.at[k % NB, pl.ds(HALF, HALF)], xssem.at[0], drsem1.at[k % NB], partner).wait_recv()
            for d in range(2):
                for sub in range(PIECES):
                    remote(sbuf.at[d, 0], rbuf.at[d, 0], dssem.at[0, d, k % NB, sub], rsem.at[d, 0], partner).wait_send()

        wait(copies_gu(sl, j))
        out = jnp.dot(b[k % NB], ring[sl], preferred_element_type=jnp.float32)
        hid[:, pl.ds(pl.multiple_of(j * 256, 256), 256)] = (jax.nn.silu(out[:, :256]) * out[:, 256:]).astype(jnp.bfloat16)
        pl.when(j < ng - 2)(lambda: start(copies_gu(sl, j + 2)))
        pl.when((j == ng - 2) & (it < K))(lambda: start(copies_q(sl)))
        pl.when((j == ng - 1) & (it < K))(lambda: start(copies_kv(sl)))
        pl.when((j >= ng - 2) & (it >= K) & (it < last))(lambda: start(copies_gu(sl, j + 2 - ng)))

    def down(it, j):
        k = it - LEAD
        sl = ring_d_place(it, j) % 2
        pl.when(j == 0)(lambda: exchanged(1, k))
        wait(copies_d(sl, j))
        out = jnp.dot(hid[...], ring_d[sl], preferred_element_type=jnp.float32)
        give(1, k % 2, pl.ds(pl.multiple_of(j * 512, 512), 512), out)
        pl.when(j < nd - 2)(lambda: start(copies_d(sl, j + 2)))
        pl.when((j >= nd - 2) & (it < K))(lambda: start(copies_o(sl, j + 2 - nd)))
        pl.when((j >= nd - 2) & (it >= K) & (it < last))(lambda: start(copies_d(sl, j + 2 - nd)))
        pl.when(j == nd - 1)(lambda: exchange(1, k))

    small = [pltpu.make_async_copy(gains_a, raw.at[0], csem.at[0]), pltpu.make_async_copy(gains_m, raw.at[1], csem.at[1]),
             pltpu.make_async_copy(turns, cos_sin, csem.at[2])]
    x_copy(0).start()
    start(small)
    start(copies_q(0))
    start(copies_kv(1))
    start(copies_o(0, 0))
    start(copies_o(1, 1))

    barrier = pltpu.get_barrier_semaphore()
    for there, who in ((z < CHIPS - 1, device(z + 1, c)), (z > 0, device(z - 1, c)), (z >= 0, partner)):
        pl.when(there)(functools.partial(pl.semaphore_signal, barrier, inc=1, device_id=who, device_id_type=MESH))
    peers = jnp.where((z > 0) & (z < CHIPS - 1), 3, 2)

    wait(small)
    for n in range(0, d_model, 128):
        for of, gain in enumerate((gain_a, gain_m)):
            gain[:, pl.ds(n, 128)] = raw[of, pl.ds(n // 128, 1), :].astype(jnp.float32)

    first_att = ng + nd
    units = first_att + 6 + nw
    cost = [1.64] * ng + [0.84] * nd + [1.1, 1.1, 1.63, 0.95, 0.95, 0.95] + [0.66] * nw
    tables = []
    for it, counts in enumerate(SLOTS):
        row = [0] * units
        at = first_att if it < LEAD else 0
        ends = [first_att + 6, units] if len(counts) == 2 else [units if it < K else first_att]
        for n, end in zip(counts, ends):
            total, done, placed = sum(cost[at:end]), 0.0, 0
            for u in range(at, end):
                done += cost[u]
                row[u] = int(n * done / total + 1e-6) - placed
                placed += row[u]
            at = end
        tables.append(row)
    kinds, alike = [], []
    for row in tables:
        if row not in alike:
            alike.append(row)
        kinds.append(alike.index(row))

    def round_(it, s):
        kind = pick(it, kinds)

        def unit(u, s):
            pl.when((it == 0) & (u == first_att + 2))(lambda: pl.semaphore_wait(barrier, peers))
            pl.when(u < ng)(lambda: gate_up(it, u))
            pl.when((u >= ng) & (u < first_att))(lambda: down(it, u - ng))
            norms, heads = u - first_att, u - first_att - 4
            pl.when((norms == 0) | (norms == 1))(lambda: norm(it, (2 * norms, 2 * norms + 2)))
            pl.when(norms == 2)(lambda: project_q(it))
            pl.when(norms == 3)(lambda: project_kv(it))
            pl.when((heads == 0) | (heads == 1))(lambda: attend(it, (2 * heads, 2 * heads + 2)))
            pl.when((heads >= 2) & (u < units))(lambda: out_project(it, heads - 2))
            n = pick(kind * units + u, [n for row in alike for n in row])
            n = jnp.where(it > last, NS - s, n)
            slots(s, n)
            return s + n

        low = jnp.where(it < LEAD, first_att, 0)
        high = jnp.where(it < K, units, first_att)
        low, high = jnp.where(it > last, units, low), jnp.where(it > last, units + 1, high)
        return lax.fori_loop(low, high, unit, s)

    lax.fori_loop(0, K + LEAD + 1, round_, jnp.int32(0))

    for d in range(2):
        p = z if d == 0 else CHIPS - 1 - z

        @pl.when(p < CHIPS - 1)
        def _():
            for i in range(NJ - 4, NJ):
                remote(sbuf.at[d, 0], rbuf.at[d, 0], ssem.at[d, i % 8], rsem.at[d, 0], partner).wait_send()

        for k in (K - 2, K - 1):
            for sub in range(PIECES):
                remote(sbuf.at[d, 0], rbuf.at[d, 0], dssem.at[1, d, k % 2, sub], rsem.at[d, 0], partner).wait_send()

        @pl.when(p == 0)
        def _():
            for k in (K - 2, K - 1):
                for sub in range(PIECES):
                    pltpu.make_async_copy(held.at[k, rows_of(sub * ROWS)], y.at[rows_of(0)], lsem.at[k % 2, sub]).wait()

    for a in range(2):
        exchanged(a, K)
    for k in range(K):
        remote(y.at[pl.ds(0, HALF)], y.at[pl.ds(0, HALF)], xssem.at[0], drsem2.at[k], partner).wait_recv()


def hand_on(src, dst, buf, rsem, wsem):
    n = buf.shape[0]
    rows = src.shape[0] // n

    def part(i):
        return pl.ds(i * rows, rows)

    reads = [pltpu.make_async_copy(src.at[part(i)], buf.at[i], rsem.at[i]) for i in range(n)]
    writes = [pltpu.make_async_copy(buf.at[i], dst.at[part(i)], wsem.at[i]) for i in range(n)]
    for read in reads:
        read.start()
    for read, write in zip(reads, writes):
        read.wait()
        write.start()
    for write in writes:
        write.wait()


def handed_on(y):
    parts = 16
    return pl.pallas_call(
        hand_on,
        out_shape=jax.ShapeDtypeStruct(y.shape, y.dtype),
        in_specs=[pl.BlockSpec(memory_space=pl.ANY)],
        out_specs=pl.BlockSpec(memory_space=pl.ANY),
        scratch_shapes=[pltpu.VMEM((parts, y.shape[0] // parts, y.shape[1]), y.dtype), pltpu.SemaphoreType.DMA((parts,)),
                        pltpu.SemaphoreType.DMA((parts,))],
        compiler_params=pltpu.CompilerParams(vmem_limit_bytes=VMEM),
        cost_estimate=pl.CostEstimate(flops=0, bytes_accessed=2 * y.size * y.dtype.itemsize, transcendentals=0),
    )(y)


def layer(x, gain_a, wq, wk, wv, wo, gain_m, w_gate, w_up, w_down):
    batch, rows, d = x.shape
    ff = w_gate.shape[1]
    bf, f32 = jnp.bfloat16, jnp.float32
    half = HEAD // 2
    angle = np.arange(rows, dtype=np.float32)[:, None] * np.power(np.float32(THETA), -np.arange(half, dtype=np.float32) / np.float32(half))
    angle = angle.astype(np.float64)
    turns = jnp.asarray(np.stack([np.concatenate([np.cos(angle), np.cos(angle)], -1), np.concatenate([-np.sin(angle), np.sin(angle)], -1)]), f32)
    dma, reg = pltpu.SemaphoreType.DMA, pltpu.SemaphoreType.REGULAR
    anywhere = pl.BlockSpec(memory_space=pl.ANY)
    tokens = batch * rows
    flops = 2 * tokens * (d * (wq.shape[1] * 2 + wk.shape[1] * 2 + 3 * ff) + rows * wq.shape[1])
    out = pl.pallas_call(
        kernel,
        out_shape=jax.ShapeDtypeStruct((tokens, d), bf),
        in_specs=[anywhere] * 11,
        out_specs=anywhere,
        scratch_shapes=[
            pltpu.VMEM((2, 2, HALF, d), f32),
            pltpu.VMEM((2, 2, HALF, d), bf),
            pltpu.VMEM((2, HALF, d), bf),
            pltpu.VMEM((NB, T, d), bf),
            pltpu.VMEM((K, QUARTER, d), bf),
            pltpu.VMEM((2, 8, ROWS, d), bf),
            pltpu.VMEM((2, 4, ROWS, d), bf),
            pltpu.VMEM((2, d, 512), bf),
            pltpu.VMEM((2, ff, 512), bf),
            pltpu.VMEM((T, ff), bf),
            pltpu.VMEM((T, d), bf),
            pltpu.VMEM((T, d), bf),
            pltpu.VMEM((4, T, HEAD), bf),
            pltpu.VMEM((2 * T, HEAD), bf),
            pltpu.VMEM((2 * T, HEAD), bf),
            pltpu.VMEM((T, 4 * HEAD), bf),
            pltpu.VMEM((2, d // 128, 128), bf),
            pltpu.VMEM((1, d), f32), pltpu.VMEM((1, d), f32),
            pltpu.VMEM((2, rows, HEAD), f32),
            dma((2, 8)), dma((2, 8)),
            dma((2,)), dma((2, 2)),
            dma((2, 2, NB, PIECES)), dma((NB,)), dma((K,)), dma((2, PIECES)),
            dma((2, 2)), dma((2, 2)), dma, dma((3,)),
            reg((2,)),
        ],
        compiler_params=pltpu.CompilerParams(collective_id=0, has_side_effects=True, vmem_limit_bytes=VMEM),
        cost_estimate=pl.CostEstimate(flops=flops, bytes_accessed=8 * tokens * d, transcendentals=0),
    )(x.reshape(tokens, d), wq, wk, wv, wo, w_gate, w_up, w_down, gain_a.reshape(-1, 128), gain_m.reshape(-1, 128), turns)
    return handed_on(out).reshape(x.shape)


def solution(mesh):
    tokens, whole, columns, rows_of = P("dp", None, None), P(None), P(None, "tp"), P("tp", None)
    return jax.shard_map(
        layer,
        mesh=mesh,
        in_specs=(tokens, whole, columns, columns, columns, rows_of, whole, columns, columns, rows_of),
        out_specs=tokens,
        check_vma=False,
    )
```
